32 devices in a mesh: row: 4 (over z), col: 8 (over y, x, core).
Axes of the slice: x: 2, y: 2, z: 4, core: 2. Of those that a mesh axis runs over, the one named last changes fastest.
Arguments:
- train_points: float32 [4, 32, 4096], P('row', None, 'col'), as said below
- targets: float32 [4, 4096], P('row', 'col'), may hold values from -16 to 16
- inverse_factor: float32 [4, 4096, 1024], P('row', 'col'), as said below
- counts: int32 [4, 4], P('row'), may hold values from 512 to 1024, as said below
- membership: int32 [4, 4, 16], replicated, may hold values from 0 to 1, as said below
- test_points: float32 [16, 32, 128], P('row'), may hold values from -6 to 6
Outputs:
- pred_mean: float32 [16, 128], P('row')
- pred_var: float32 [16, 128], P('row')
The draws below stay inside these ranges and needn't reach their ends.
Inputs may be any that keep to these rules, and one draw needn't show every extreme that they name: Each expert membership[r, c, :] takes part in at least one and at most 4 blocks, exactly 4 for at least one expert, and in at most one of the 4 blocks of each owner row. `counts`: at least one expert has all 1024 points valid. `inverse_factor`: F[i, j] as in the reference program is entry (i, j) of the inverse of the lower Cholesky factor of the expert's matrix whose entries are exp(-|x_i - x_j|^2 / 32), plus 0.1 on the diagonal, for valid i and j, and that is the identity elsewhere. `train_points`: each expert's 1024 points are drawn independently of the other experts' points.
All inputs are finite; a program needn't handle non-finite values.
Results may differ from the reference program's by a relative error of at most 0.0003.
Values sent between devices are 32-bit elements; how exact they have to be, the bound alone decides.
A program may use at most 64 MiB of HBM per device.

```python
import jax
import jax.numpy as jnp
from jax import lax

D = 32
N_PTS = 1024
BS = 128
BPR = 4
MAXB = 4
ECOL = 4
NBLK = 16
N_ROW = 4


SIGNAL = 1.0


NOISE = 0.1


def expert_points(key):
    experts_all = N_ROW * ECOL
    point_key = jax.random.fold_in(key, 11)
    points = jax.random.normal(point_key, (experts_all, N_PTS, D), jnp.float32)
    return points


def expert_counts(key):
    experts_all = N_ROW * ECOL
    drawn = jax.random.randint(jax.random.fold_in(key, 21), (experts_all,), N_PTS // 2, N_PTS + 1, jnp.int32)
    fullest = jax.random.randint(jax.random.fold_in(key, 22), (), 0, experts_all, jnp.int32)
    return drawn.at[fullest].set(N_PTS)


def factor_one(points, valid_count):
    row_valid = jnp.arange(N_PTS, dtype=jnp.int32) < valid_count
    squares = jnp.sum(points * points, axis=1)
    products = jnp.dot(points, points.T, precision=lax.Precision.HIGHEST)
    spread = squares[:, None] + squares[None, :] - 2.0 * products
    kernel = SIGNAL * jnp.exp(-spread / D)
    both_valid = row_valid[:, None] & row_valid[None, :]
    diagonal = jnp.where(row_valid, NOISE, 1.0).astype(jnp.float32)
    matrix = jnp.where(both_valid, kernel, 0.0) + jnp.diag(diagonal)
    lower = jnp.linalg.cholesky(matrix)
    identity = jnp.eye(N_PTS, dtype=jnp.float32)
    return lax.linalg.triangular_solve(lower, identity, left_side=True, lower=True)


def draw_train_points(key, part):
    experts_all = N_ROW * ECOL
    points = expert_points(key)
    stored = points.reshape(experts_all, N_PTS // 2, 2, D).transpose(0, 2, 1, 3).reshape(experts_all, N_PTS, D)
    return stored.reshape(N_ROW, ECOL, N_PTS, D).transpose(0, 3, 1, 2).reshape(N_ROW, D, ECOL * N_PTS)


def draw_inverse_factor(key, part):
    experts_all = N_ROW * ECOL
    points = expert_points(key)
    valid_counts = expert_counts(key)
    factors = lax.map(lambda expert_items: factor_one(expert_items[0], expert_items[1]), (points, valid_counts))
    stored = factors.reshape(experts_all, N_PTS // 2, 2, N_PTS).transpose(0, 2, 1, 3)
    return stored.reshape(N_ROW, ECOL * N_PTS, N_PTS)


def draw_counts(key, part):
    return expert_counts(key).reshape(N_ROW, ECOL)


def draw_membership(key, part):
    experts_all = N_ROW * ECOL
    base_key = jax.random.fold_in(key, 31)
    is_busy = jax.random.randint(jax.random.fold_in(base_key, 1), (experts_all,), 0, 8, jnp.int32) == 0
    light = jax.random.randint(jax.random.fold_in(base_key, 2), (experts_all,), 1, MAXB // 2 + 1, jnp.int32)
    taken = jnp.where(is_busy, MAXB, light).astype(jnp.int32)
    fullest = jax.random.randint(jax.random.fold_in(base_key, 3), (), 0, experts_all, jnp.int32)
    taken = taken.at[fullest].set(MAXB)
    expert_keys = jax.random.split(jax.random.fold_in(base_key, 4), experts_all)
    orders = jax.vmap(lambda one_key: jax.random.permutation(one_key, N_ROW))(expert_keys)
    places = jnp.argsort(orders, axis=1).astype(jnp.int32)
    chosen_rows = places < taken[:, None]
    block_picks = jax.random.randint(jax.random.fold_in(base_key, 5), (experts_all, N_ROW), 0, BPR, jnp.int32)
    inside = block_picks[:, :, None] == jnp.arange(BPR, dtype=jnp.int32)[None, None, :]
    member = chosen_rows[:, :, None] & inside
    return member.reshape(N_ROW, ECOL, N_ROW * BPR).astype(jnp.int32)


def block_scale(stream_key, dims, cuts, least, top_value):
    def one(axis_at, parts):
        heights = jax.random.uniform(jax.random.fold_in(jax.random.fold_in(stream_key, 6), axis_at), (parts,), jnp.float32, least / len(cuts), top_value / len(cuts))
        return jnp.repeat(jnp.exp(heights), dims[axis_at] // parts).reshape((-1,) + (1,) * (len(dims) - axis_at - 1))

    loudness = one(*cuts[0])
    for cut in cuts[1:]:
        loudness = loudness * one(*cut)
    return loudness


def bell_draw(rng, dims, deviation, limit, shards=(), kind=jnp.bfloat16):
    gain = block_scale(rng, dims, shards, -0.22, 0.18) if shards else 1.0
    values = jax.random.normal(rng, dims, jnp.float32) * deviation * gain
    return jnp.minimum(jnp.maximum(values, -limit), limit).astype(kind)


def setup_inputs(seed: int = 0) -> dict:
    streams_of = jax.random.split(jax.random.key(seed), 7)
    return {
        "train_points": draw_train_points(jax.random.fold_in(streams_of[6], 71), 0),
        "targets": bell_draw(streams_of[1], (N_ROW, ECOL * N_PTS), 3.0, 16.0, ((0, 4), (1, 8)), jnp.float32),
        "inverse_factor": draw_inverse_factor(jax.random.fold_in(streams_of[6], 71), 0),
        "counts": draw_counts(jax.random.fold_in(streams_of[6], 71), 0),
        "membership": draw_membership(jax.random.fold_in(streams_of[6], 71), 0),
        "test_points": bell_draw(streams_of[5], (NBLK, D, BS), 1.0, 6.0, ((0, 4),), jnp.float32),
    }


SIGNAL = 1.0
NOISE = 0.1
HIGHEST = lax.Precision.HIGHEST

def cross_kernel(train_cols, test_cols, squared_scale):
    products = jnp.einsum('dn,dp->np', train_cols, test_cols, precision=HIGHEST)
    spread = jnp.sum(train_cols * train_cols, axis=0)[:, None] + jnp.sum(test_cols * test_cols, axis=0)[None, :] - 2.0 * products
    return SIGNAL * jnp.exp(-0.5 * spread / squared_scale)

def slot_table(member, slot_count):
    member_flags = member.astype(jnp.int32)
    before = jnp.cumsum(member_flags) - member_flags
    slot_ids = jnp.arange(slot_count, dtype=jnp.int32)[:, None]
    picked = ((member_flags[None, :] == 1) & (before[None, :] == slot_ids)).astype(jnp.int32)
    chosen = jnp.sum(picked * jnp.arange(member.shape[0], dtype=jnp.int32)[None, :], axis=1).astype(jnp.int32)
    return (picked.astype(jnp.float32), chosen)

def weigh_expert(mean_part, quad_part):
    variance = NOISE + jnp.maximum(SIGNAL - quad_part, 0.0)
    entropy_gap = 0.5 * (jnp.log(SIGNAL + NOISE) - jnp.log(variance))
    weight = entropy_gap / variance
    return (weight * mean_part, weight)

def reference(train_points, targets, inverse_factor, counts, membership, test_points):
    features = train_points.shape[1]
    squared_scale = 0.5 * features
    experts_all = N_ROW * ECOL
    half_pts = N_PTS // 2
    train_all = train_points.reshape(N_ROW, features, ECOL, N_PTS).transpose(0, 2, 1, 3).reshape(experts_all, features, 2, half_pts)
    train_all = train_all.transpose(0, 1, 3, 2).reshape(experts_all, features, N_PTS)
    target_all = targets.reshape(experts_all, 2, half_pts).transpose(0, 2, 1).reshape(experts_all, N_PTS)
    factor_all = inverse_factor.reshape(experts_all, 2, half_pts, N_PTS).transpose(0, 2, 1, 3).reshape(experts_all, N_PTS, N_PTS)
    count_all = counts.reshape(experts_all)
    member_all = membership.reshape(experts_all, NBLK)

    def accumulate(totals, expert_items):
        train_cols, target_col, factor, valid_count, member = expert_items
        picked, chosen = slot_table(member, MAXB)
        test_cols = test_points[chosen].transpose(1, 0, 2).reshape(features, MAXB * BS)
        row_valid = jnp.arange(N_PTS, dtype=jnp.int32) < valid_count
        kernel = jnp.where(row_valid[:, None], cross_kernel(train_cols, test_cols, squared_scale), 0.0)
        solved = jnp.dot(factor.astype(jnp.float32), kernel.astype(jnp.float32), precision=HIGHEST, preferred_element_type=jnp.float32)
        whitened = jnp.dot(factor.astype(jnp.float32), target_col.astype(jnp.float32), precision=HIGHEST, preferred_element_type=jnp.float32)
        mean_part = jnp.dot(whitened.astype(jnp.float32), solved.astype(jnp.float32), precision=HIGHEST, preferred_element_type=jnp.float32)
        quad_part = jnp.sum(solved * solved, axis=0)
        weighted, weight = weigh_expert(mean_part, quad_part)
        dense_num = jnp.einsum('sb,sp->bp', picked, weighted.reshape(MAXB, BS), precision=HIGHEST)
        dense_wgt = jnp.einsum('sb,sp->bp', picked, weight.reshape(MAXB, BS), precision=HIGHEST)
        return ((totals[0] + dense_num, totals[1] + dense_wgt), None)
    start = (jnp.zeros((NBLK, BS), jnp.float32), jnp.zeros((NBLK, BS), jnp.float32))
    totals, _ = lax.scan(accumulate, start, (train_all, target_all, factor_all, count_all, member_all))
    precision_sum = 1.0 / (SIGNAL + NOISE) + totals[1]
    return (totals[0] / precision_sum, 1.0 / precision_sum)
```

```python
import functools

import jax
import jax.numpy as jnp
from jax import lax
from jax.experimental import pallas as pl
from jax.experimental.pallas import tpu as pltpu
from jax.sharding import PartitionSpec as P

SIGNAL = 1.0
NOISE = 0.1
F32 = jnp.float32
BF16 = jnp.bfloat16
MESH = pl.DeviceIdType.MESH


def high_low(value):
    high = value.astype(BF16)
    return high, (value - high.astype(F32)).astype(BF16)


def expert_kernel(
    rows, cols,
    counts_hbm, member_hbm, train_ref, target_ref, factor_ref, test_ref,
    sums_ref,
    factor_buf, own_x, own_y, tests, other_x, other_y, sent_tests, got_tests,
    factor_high, factor_low, nat_a, nat_b, points, k_high, k_low,
    sent_parts, got_parts, taken_by, sent_bytes, alpha, counts_ref, member_ref,
    local_sems, x_send, x_recv, t_send, t_recv, p_send, p_recv,
):
    row = lax.axis_index("row")
    col = lax.axis_index("col")
    parity = col % 2
    expert = col // 2
    experts = cols // 2
    blocks, features, length = tests.shape
    half = own_x.shape[1]
    partner = (row, expert * 2 + 1 - parity)

    others = [lax.rem(row + d, rows) for d in range(1, rows)]
    mates = [lax.rem(expert + d, experts) for d in range(1, experts)]
    barrier = pltpu.get_barrier_semaphore()
    peers = [partner]
    for r in others:
        peers += [(r, expert * 2), (r, expert * 2 + 1)]
    for c in mates:
        peers += [(row, c * 2), (row, c * 2 + 1)]
    for peer in peers:
        pl.semaphore_signal(barrier, inc=1, device_id=peer, device_id_type=MESH)

    load_member = pltpu.make_async_copy(member_hbm, member_ref, local_sems.at[4])
    load_counts = pltpu.make_async_copy(counts_hbm, counts_ref, local_sems.at[5])
    load_tests = pltpu.make_async_copy(test_ref, tests, local_sems.at[0])
    load_member.start()
    load_x = pltpu.make_async_copy(train_ref.at[0], own_x, local_sems.at[1])
    load_y = pltpu.make_async_copy(target_ref, own_y, local_sems.at[2])
    load_f = pltpu.make_async_copy(factor_ref.at[0], factor_buf, local_sems.at[3])
    load_tests.start()
    load_x.start()
    load_y.start()
    load_counts.start()
    load_f.start()

    def chosen_in(row_at, owner):
        at = jnp.int32(0)
        for j in range(1, blocks):
            at = at + j * member_ref[row_at, expert, owner * blocks + j]
        return at

    load_member.wait()
    load_tests.wait()
    for d, r in enumerate(others):
        sent_tests[d] = tests[chosen_in(r, row)]
    pl.semaphore_wait(barrier, len(peers))

    def remote(src, dst, send, recv, peer):
        copy = pltpu.make_async_remote_copy(
            src_ref=src, dst_ref=dst, send_sem=send, recv_sem=recv,
            device_id=peer, device_id_type=MESH,
        )
        copy.start()
        return copy

    load_x.wait()
    load_y.wait()
    x_copy = remote(own_x, other_x, x_send.at[0], x_recv.at[0], partner)
    y_copy = remote(own_y, other_y, x_send.at[1], x_recv.at[1], partner)
    test_copies = [
        remote(sent_tests.at[d], got_tests.at[d], t_send.at[d], t_recv.at[d],
               (r, col))
        for d, r in enumerate(others)
    ]

    def stacked(x, y):
        xh = x.astype(BF16).astype(F32)
        xl = x - xh
        x2 = jnp.sum(x * x, axis=0, keepdims=True)
        a = x2.astype(BF16).astype(F32)
        b = (x2 - a).astype(BF16).astype(F32)
        c = x2 - a - b
        yh = y.astype(BF16).astype(F32)
        yl = y - yh
        at = lax.broadcasted_iota(jnp.int32, (8, half), 0)
        tail = jnp.zeros((8, half), F32)
        for i, v in enumerate((a, b, c, yh, yl)):
            tail = jnp.where(at == i, v, tail)
        first = jnp.concatenate([xh, xl, xh, xl], axis=0)
        last = jnp.concatenate([tail, jnp.zeros((120, half), F32)], axis=0)
        return first.T, last.T

    def put(a, b, offset):
        nat_a[pl.ds(offset, half, stride=2), :] = a
        nat_b[pl.ds(offset, half, stride=2), :] = b

    a, b = stacked(own_x[...], own_y[...])

    @pl.when(parity == 0)
    def _():
        put(a, b, 0)

    @pl.when(parity == 1)
    def _():
        put(a, b, 1)

    load_f.wait()
    fh, fl = high_low(factor_buf[...])
    factor_high[...] = fh
    factor_low[...] = fl

    x_copy.wait_recv()
    y_copy.wait_recv()
    a2, b2 = stacked(other_x[...], other_y[...])

    @pl.when(parity == 1)
    def _():
        put(a2, b2, 0)

    @pl.when(parity == 0)
    def _():
        put(a2, b2, 1)

    points[:, :128] = nat_a[...].astype(BF16)
    points[:, 128:] = nat_b[...].astype(BF16)
    solved_y = jnp.dot(factor_high[...], points[:, 128:], preferred_element_type=F32)
    solved_y += jnp.dot(factor_low[...], points[:, 128:], preferred_element_type=F32)
    whitened = solved_y[:, 3:4] + solved_y[:, 4:5]
    solved_back = jnp.sum(factor_buf[...] * whitened, axis=0, keepdims=True)
    for i in range(0, 2 * half, 128):
        alpha[i:i + 128, :] = jnp.broadcast_to(solved_back[:, i:i + 128], (128, 128)).T

    load_counts.wait()
    valid = counts_ref[0, expert]
    pair = 2 * length
    tail_at = lax.broadcasted_iota(jnp.int32, (128, pair), 0)
    tail_t = jnp.where(tail_at < 3, -1.0, 0.0).astype(BF16)
    chunk = 128
    order = [None] + list(range(rows - 1))
    owners = [row] + [lax.rem(row + rows - d - 1, rows) for d in range(rows - 1)]
    for first in range(0, rows, 2):
        taken = []
        for s in (first, first + 1):
            d = order[s]
            if d is None:
                taken.append(tests[chosen_in(row, row)])
            else:
                test_copies[d].wait_recv()
                taken.append(got_tests[d])
        t = jnp.concatenate(taken, axis=1)
        th, tl = high_low(2.0 * t)
        t2 = jnp.sum(t * t, axis=0, keepdims=True)
        rhs = jnp.concatenate([th, th, tl, tl, tail_t], axis=0)
        mean = jnp.zeros((1, pair), F32)
        for i in range(0, 2 * half, chunk):
            e = jnp.dot(points[i:i + chunk, :], rhs, preferred_element_type=F32) - t2
            k = jnp.exp(e * (1.0 / features))
            at = lax.broadcasted_iota(jnp.int32, (chunk, pair), 0) + i
            k = jnp.where(at < valid, SIGNAL * k, 0.0)
            along = alpha[i:i + chunk, :]
            mean += jnp.sum(k * jnp.concatenate([along, along], axis=1), axis=0, keepdims=True)
            kh, kl = high_low(k)
            k_high[i:i + chunk, :] = kh
            k_low[i:i + chunk, :] = kl
        solved = jnp.dot(factor_high[...], k_high[...], preferred_element_type=F32)
        solved += jnp.dot(factor_low[...], k_high[...], preferred_element_type=F32)
        solved += jnp.dot(factor_high[...], k_low[...], preferred_element_type=F32)
        quad = jnp.sum(solved * solved, axis=0, keepdims=True)
        for n, s in enumerate((first, first + 1)):
            lanes = slice(n * length, (n + 1) * length)
            d = order[s]
            sent_parts[s, 0:1, :] = mean[:, lanes]
            sent_parts[s, 1:2, :] = quad[:, lanes]
            mine = got_parts.at[expert, parity, row]
            if d is None:
                keep = pltpu.make_async_copy(sent_parts.at[s], mine, p_recv.at[0])
                keep.start()
                targets = [partner]
                for c in mates:
                    targets += [(row, c * 2), (row, c * 2 + 1)]
            else:
                targets = [(owners[s], lax.rem(col + c, cols)) for c in range(cols)]
            for target in targets:
                remote(sent_parts.at[s], mine, p_send.at[s], p_recv.at[0], target)

    for j in range(blocks):
        for e in range(experts):
            for r in range(rows):
                on = member_ref[r, e, row * blocks + j]
                n = e * rows + r
                taken_by[j, n:n + 1, :] = jnp.full((1, length), on, jnp.int32).astype(F32)

    pltpu.make_async_copy(got_parts, got_parts, p_recv.at[0]).wait()
    total = got_parts[:, 0] + got_parts[:, 1]
    total = total.reshape(experts * rows, 2, length)
    mean = total[:, 0, :]
    quad = total[:, 1, :]
    variance = NOISE + jnp.maximum(SIGNAL - quad, 0.0)
    gap = 0.5 * (jnp.log(jnp.full_like(variance, SIGNAL + NOISE)) - jnp.log(variance))
    weight = gap / variance
    weighted = weight * mean
    for j in range(blocks):
        on = taken_by[j] > 0.5
        sums_ref[j:j + 1, :] = jnp.sum(jnp.where(on, weighted, 0.0), axis=0, keepdims=True)
        sums_ref[blocks + j:blocks + j + 1, :] = jnp.sum(
            jnp.where(on, weight, 0.0), axis=0, keepdims=True)
    x_copy.wait_send()
    y_copy.wait_send()
    for copy in test_copies:
        copy.wait_send()
    for s in range(rows):
        sent = cols - 1 if order[s] is None else cols
        flat = sent_bytes.at[pl.ds(0, sent)]
        pltpu.make_async_copy(flat, flat, p_send.at[s]).wait()


def on_device(rows, cols, train_points, targets, inverse_factor, counts, membership, test_points):
    features, half = train_points.shape[1:]
    blocks, _, length = test_points.shape
    points = inverse_factor.shape[2]
    experts = cols // 2
    vmem, dma = pltpu.VMEM, pltpu.SemaphoreType.DMA
    anywhere = pl.BlockSpec(memory_space=pltpu.HBM)
    sums = pl.pallas_call(
        functools.partial(expert_kernel, rows, cols),
        out_shape=jax.ShapeDtypeStruct((2 * blocks, length), F32),
        in_specs=[anywhere] * 6,
        out_specs=pl.BlockSpec(memory_space=pltpu.VMEM),
        scratch_shapes=[
            vmem((half, points), F32),
            vmem((features, half), F32),
            vmem((1, half), F32),
            vmem((blocks, features, length), F32),
            vmem((features, half), F32),
            vmem((1, half), F32),
            vmem((rows - 1, features, length), F32),
            vmem((rows - 1, features, length), F32),
            vmem((half, points), BF16),
            vmem((half, points), BF16),
            vmem((points, 128), F32),
            vmem((points, 128), F32),
            vmem((points, 256), BF16),
            vmem((points, 2 * length), BF16),
            vmem((points, 2 * length), BF16),
            vmem((rows, 2, length), F32),
            vmem((experts, 2, rows, 2, length), F32),
            vmem((blocks, experts * rows, length), F32),
            vmem((cols, 2, length), F32),
            vmem((points, 128), F32),
            pltpu.SMEM(counts.shape, jnp.int32),
            pltpu.SMEM(membership.shape, jnp.int32),
            dma((6,)),
            dma((2,)),
            dma((2,)),
            dma((rows - 1,)),
            dma((rows - 1,)),
            dma((rows,)),
            dma((1,)),
        ],
        compiler_params=pltpu.CompilerParams(
            collective_id=0, has_side_effects=True
        ),
    )(counts, membership, train_points, targets, inverse_factor, test_points)
    precision_sum = 1.0 / (SIGNAL + NOISE) + sums[blocks:]
    return (sums[:blocks] / precision_sum, 1.0 / precision_sum)


def solution(mesh):
    in_specs = (
        P("row", None, "col"),
        P("row", "col"),
        P("row", "col", None),
        P("row", None),
        P(),
        P("row", None, None),
    )
    out_specs = (P("row", None), P("row", None))
    body = functools.partial(on_device, mesh.shape["row"], mesh.shape["col"])
    return jax.shard_map(
        body, mesh=mesh, in_specs=in_specs, out_specs=out_specs, check_vma=False
    )
```

```python
import functools

import jax
import jax.numpy as jnp
from jax import lax
from jax.experimental import pallas as pl
from jax.experimental.pallas import tpu as pltpu
from jax.sharding import PartitionSpec as P

SIGNAL = 1.0
NOISE = 0.1
F32 = jnp.float32
BF16 = jnp.bfloat16
MESH = pl.DeviceIdType.MESH


def high_low(value):
    high = value.astype(BF16)
    return high, (value - high.astype(F32)).astype(BF16)


def expert_kernel(
    rows, cols,
    counts_hbm, member_hbm, train_ref, target_ref, factor_ref, test_ref,
    sums_ref,
    factor_buf, own_x, own_y, tests, other_x, other_y, sent_tests, got_tests,
    factor_high, factor_low, nat_a, nat_b, points, k_high, k_low,
    sent_parts, got_parts, taken_by, sent_bytes, alpha, counts_ref, member_ref,
    local_sems, x_send, x_recv, t_send, t_recv, p_send, p_recv,
):
    row = lax.axis_index("row")
    col = lax.axis_index("col")
    parity = col % 2
    expert = col // 2
    experts = cols // 2
    blocks, features, length = tests.shape
    half = own_x.shape[1]
    partner = (row, expert * 2 + 1 - parity)

    others = [lax.rem(row + d, rows) for d in range(1, rows)]
    mates = [lax.rem(expert + d, experts) for d in range(1, experts)]
    barrier = pltpu.get_barrier_semaphore()
    peers = [partner]
    for r in others:
        peers += [(r, expert * 2), (r, expert * 2 + 1)]
    for c in mates:
        peers += [(row, c * 2), (row, c * 2 + 1)]
    for peer in peers:
        pl.semaphore_signal(barrier, inc=1, device_id=peer, device_id_type=MESH)

    load_member = pltpu.make_async_copy(member_hbm, member_ref, local_sems.at[4])
    load_counts = pltpu.make_async_copy(counts_hbm, counts_ref, local_sems.at[5])
    load_tests = pltpu.make_async_copy(test_ref, tests, local_sems.at[0])
    load_member.start()
    load_x = pltpu.make_async_copy(train_ref.at[0], own_x, local_sems.at[1])
    load_y = pltpu.make_async_copy(target_ref, own_y, local_sems.at[2])
    load_f = pltpu.make_async_copy(factor_ref.at[0], factor_buf, local_sems.at[3])
    load_tests.start()
    load_x.start()
    load_y.start()
    load_counts.start()
    load_f.start()

    def chosen_in(row_at, owner):
        at = jnp.int32(0)
        for j in range(1, blocks):
            at = at + j * member_ref[row_at, expert, owner * blocks + j]
        return at

    load_member.wait()
    load_tests.wait()
    for d, r in enumerate(others):
        sent_tests[d] = tests[chosen_in(r, row)]
    pl.semaphore_wait(barrier, len(peers))

    def remote(src, dst, send, recv, peer):
        copy = pltpu.make_async_remote_copy(
            src_ref=src, dst_ref=dst, send_sem=send, recv_sem=recv,
            device_id=peer, device_id_type=MESH,
        )
        copy.start()
        return copy

    load_x.wait()
    load_y.wait()
    x_copy = remote(own_x, other_x, x_send.at[0], x_recv.at[0], partner)
    y_copy = remote(own_y, other_y, x_send.at[1], x_recv.at[1], partner)
    test_copies = [
        remote(sent_tests.at[d], got_tests.at[d], t_send.at[d], t_recv.at[d],
               (r, col))
        for d, r in enumerate(others)
    ]

    def stacked(x, y):
        xh = x.astype(BF16).astype(F32)
        xl = x - xh
        x2 = jnp.sum(x * x, axis=0, keepdims=True)
        a = x2.astype(BF16).astype(F32)
        b = (x2 - a).astype(BF16).astype(F32)
        c = x2 - a - b
        yh = y.astype(BF16).astype(F32)
        yl = y - yh
        at = lax.broadcasted_iota(jnp.int32, (8, half), 0)
        tail = jnp.zeros((8, half), F32)
        for i, v in enumerate((a, b, c, yh, yl)):
            tail = jnp.where(at == i, v, tail)
        first = jnp.concatenate([xh, xl, xh, xl], axis=0)
        last = jnp.concatenate([tail, jnp.zeros((120, half), F32)], axis=0)
        return first.T, last.T

    def put(a, b, offset):
        nat_a[pl.ds(offset, half, stride=2), :] = a
        nat_b[pl.ds(offset, half, stride=2), :] = b

    a, b = stacked(own_x[...], own_y[...])

    @pl.when(parity == 0)
    def _():
        put(a, b, 0)

    @pl.when(parity == 1)
    def _():
        put(a, b, 1)

    load_f.wait()
    fh, fl = high_low(factor_buf[...])
    factor_high[...] = fh
    factor_low[...] = fl

    x_copy.wait_recv()
    y_copy.wait_recv()
    a2, b2 = stacked(other_x[...], other_y[...])

    @pl.when(parity == 1)
    def _():
        put(a2, b2, 0)

    @pl.when(parity == 0)
    def _():
        put(a2, b2, 1)

    points[:, :128] = nat_a[...].astype(BF16)
    points[:, 128:] = nat_b[...].astype(BF16)
    solved_y = jnp.dot(factor_high[...], points[:, 128:], preferred_element_type=F32)
    solved_y += jnp.dot(factor_low[...], points[:, 128:], preferred_element_type=F32)
    whitened = solved_y[:, 3:4] + solved_y[:, 4:5]
    solved_back = jnp.sum(factor_buf[...] * whitened, axis=0, keepdims=True)
    for i in range(0, 2 * half, 128):
        alpha[i:i + 128, :] = jnp.broadcast_to(solved_back[:, i:i + 128], (128, 128)).T

    load_counts.wait()
    valid = counts_ref[0, expert]
    pair = 2 * length
    tail_at = lax.broadcasted_iota(jnp.int32, (128, pair), 0)
    tail_t = jnp.where(tail_at < 3, -1.0, 0.0).astype(BF16)
    chunk = 128
    order = [None] + list(range(rows - 1))
    owners = [row] + [lax.rem(row + rows - d - 1, rows) for d in range(rows - 1)]
    groups = [(0,)] + [tuple(range(s, min(s + 2, rows))) for s in range(1, rows, 2)]
    for group in groups:
        wide = len(group) * length
        taken = []
        for s in group:
            d = order[s]
            if d is None:
                taken.append(tests[chosen_in(row, row)])
            else:
                test_copies[d].wait_recv()
                taken.append(got_tests[d])
        t = jnp.concatenate(taken, axis=1)
        th, tl = high_low(2.0 * t)
        t2 = jnp.sum(t * t, axis=0, keepdims=True)
        rhs = jnp.concatenate([th, th, tl, tl, tail_t[:, :wide]], axis=0)
        mean = jnp.zeros((1, wide), F32)
        for i in range(0, 2 * half, chunk):
            e = jnp.dot(points[i:i + chunk, :], rhs, preferred_element_type=F32) - t2
            k = jnp.exp(e * (1.0 / features))
            at = lax.broadcasted_iota(jnp.int32, (chunk, wide), 0) + i
            k = jnp.where(at < valid, SIGNAL * k, 0.0)
            along = alpha[i:i + chunk, :]
            mean += jnp.sum(k * jnp.concatenate([along] * len(group), axis=1), axis=0, keepdims=True)
            kh, kl = high_low(k)
            k_high[i:i + chunk, :wide] = kh
            k_low[i:i + chunk, :wide] = kl
        solved = jnp.dot(factor_high[...], k_high[:, :wide], preferred_element_type=F32)
        solved += jnp.dot(factor_low[...], k_high[:, :wide], preferred_element_type=F32)
        solved += jnp.dot(factor_high[...], k_low[:, :wide], preferred_element_type=F32)
        quad = jnp.sum(solved * solved, axis=0, keepdims=True)
        for n, s in enumerate(group):
            lanes = slice(n * length, (n + 1) * length)
            d = order[s]
            sent_parts[s, 0:1, :] = mean[:, lanes]
            sent_parts[s, 1:2, :] = quad[:, lanes]
            mine = got_parts.at[expert, parity, row]
            if d is None:
                keep = pltpu.make_async_copy(sent_parts.at[s], mine, p_recv.at[0])
                keep.start()
                targets = [partner]
                for c in mates:
                    targets += [(row, c * 2), (row, c * 2 + 1)]
            else:
                targets = [(owners[s], lax.rem(col + c, cols)) for c in range(cols)]
            for target in targets:
                remote(sent_parts.at[s], mine, p_send.at[s], p_recv.at[0], target)

    for j in range(blocks):
        for e in range(experts):
            for r in range(rows):
                on = member_ref[r, e, row * blocks + j]
                n = e * rows + r
                taken_by[j, n:n + 1, :] = jnp.full((1, length), on, jnp.int32).astype(F32)

    pltpu.make_async_copy(got_parts, got_parts, p_recv.at[0]).wait()
    total = got_parts[:, 0] + got_parts[:, 1]
    total = total.reshape(experts * rows, 2, length)
    mean = total[:, 0, :]
    quad = total[:, 1, :]
    variance = NOISE + jnp.maximum(SIGNAL - quad, 0.0)
    gap = 0.5 * (jnp.log(jnp.full_like(variance, SIGNAL + NOISE)) - jnp.log(variance))
    weight = gap / variance
    weighted = weight * mean
    for j in range(blocks):
        on = taken_by[j] > 0.5
        sums_ref[j:j + 1, :] = jnp.sum(jnp.where(on, weighted, 0.0), axis=0, keepdims=True)
        sums_ref[blocks + j:blocks + j + 1, :] = jnp.sum(
            jnp.where(on, weight, 0.0), axis=0, keepdims=True)
    x_copy.wait_send()
    y_copy.wait_send()
    for copy in test_copies:
        copy.wait_send()
    for s in range(rows):
        sent = cols - 1 if order[s] is None else cols
        flat = sent_bytes.at[pl.ds(0, sent)]
        pltpu.make_async_copy(flat, flat, p_send.at[s]).wait()


def on_device(rows, cols, train_points, targets, inverse_factor, counts, membership, test_points):
    features, half = train_points.shape[1:]
    blocks, _, length = test_points.shape
    points = inverse_factor.shape[2]
    experts = cols // 2
    vmem, dma = pltpu.VMEM, pltpu.SemaphoreType.DMA
    anywhere = pl.BlockSpec(memory_space=pltpu.HBM)
    sums = pl.pallas_call(
        functools.partial(expert_kernel, rows, cols),
        out_shape=jax.ShapeDtypeStruct((2 * blocks, length), F32),
        in_specs=[anywhere] * 6,
        out_specs=pl.BlockSpec(memory_space=pltpu.VMEM),
        scratch_shapes=[
            vmem((half, points), F32),
            vmem((features, half), F32),
            vmem((1, half), F32),
            vmem((blocks, features, length), F32),
            vmem((features, half), F32),
            vmem((1, half), F32),
            vmem((rows - 1, features, length), F32),
            vmem((rows - 1, features, length), F32),
            vmem((half, points), BF16),
            vmem((half, points), BF16),
            vmem((points, 128), F32),
            vmem((points, 128), F32),
            vmem((points, 256), BF16),
            vmem((points, 2 * length), BF16),
            vmem((points, 2 * length), BF16),
            vmem((rows, 2, length), F32),
            vmem((experts, 2, rows, 2, length), F32),
            vmem((blocks, experts * rows, length), F32),
            vmem((cols, 2, length), F32),
            vmem((points, 128), F32),
            pltpu.SMEM(counts.shape, jnp.int32),
            pltpu.SMEM(membership.shape, jnp.int32),
            dma((6,)),
            dma((2,)),
            dma((2,)),
            dma((rows - 1,)),
            dma((rows - 1,)),
            dma((rows,)),
            dma((1,)),
        ],
        compiler_params=pltpu.CompilerParams(
            collective_id=0, has_side_effects=True
        ),
    )(counts, membership, train_points, targets, inverse_factor, test_points)
    precision_sum = 1.0 / (SIGNAL + NOISE) + sums[blocks:]
    return (sums[:blocks] / precision_sum, 1.0 / precision_sum)


def solution(mesh):
    in_specs = (
        P("row", None, "col"),
        P("row", "col"),
        P("row", "col", None),
        P("row", None),
        P(),
        P("row", None, None),
    )
    out_specs = (P("row", None), P("row", None))
    body = functools.partial(on_device, mesh.shape["row"], mesh.shape["col"])
    return jax.shard_map(
        body, mesh=mesh, in_specs=in_specs, out_specs=out_specs, check_vma=False
    )
```
